256 devices in a mesh: video: 4 (over y), seq: 64 (over z, x, core).
Axes of the slice: x: 4, y: 4, z: 8, core: 2. Of those that a mesh axis runs over, the one named last changes fastest.
Arguments:
- queries: bfloat16 [32768, 2048], P(('video', 'seq')), parts along dimension 0, may hold values from -80 to 80
- keys: bfloat16 [32768, 2048], P(('video', 'seq')), parts along dimension 0, may hold values from -5 to 5
- values: bfloat16 [32768, 2048], P(('video', 'seq')), parts along dimension 0, may hold values from -6 to 6
- history: bfloat16 [16, 16384], P(None, ('video', 'seq')), parts along dimension 1, may hold values from -6 to 6
- levels: int32 [256], P('video'), parts along dimension 0, may hold values from 2 to 16, as said below
- patch_two: bfloat16 [32, 3072], replicated, may hold values from -1 to 1
- patch_four: bfloat16 [64, 3072], replicated, may hold values from -0.75 to 0.75
- patch_sixteen: bfloat16 [256, 3072], replicated, may hold values from -0.375 to 0.375
- mod_scale: float32 [3072], replicated, may hold values from -0.5 to 0.5
- mod_shift: float32 [3072], replicated, may hold values from -4 to 4
- kv_weight: bfloat16 [3072, 4096], P(None, 'seq'), may hold values from -0.109375 to 0.109375
- key_gain: float32 [128], replicated, may hold values from 0.5 to 2
Outputs:
- attended: bfloat16 [32768, 2048], P(('video', 'seq')), parts along dimension 0
The draws below stay inside these ranges and needn't reach their ends.
There are 4 independent parts, one for each index of `video`. The reference program is written for one: setup_inputs(seed, part) draws one part's arguments, and reference() takes and returns one part's arrays. A program takes and returns all parts, laid end to end along the dimension named above; an argument that names none is the same for every part. Nothing has to cross between parts.
Inputs may be any that keep to these rules, and one draw needn't show every extreme that they name: `levels`: each aligned group of four devices holds the factors 2, 4, 4 and 16 in some order, so that one device's block gives at most 32 history tokens.
All inputs are finite; a program needn't handle non-finite values.
Results may differ from the reference program's by a relative error of at most 0.0034.
Values may be sent and summed in bfloat16 or wider, within the bound.
No kernel may reach another device: no remote copies, remote signals or barrier semaphores. Data moves between devices by JAX's collectives and lax.ppermute only.
A program may use at most 128 MiB of HBM per device.

```python
import math
import jax
import jax.numpy as jnp
from jax import lax

D = 3072
HEADS = 16
HD = 128
LATC = 16
HPOS = 64
TOKENS = 8192
HIST = 1088
N_SEQ = 64


def paired_rows(key):
    base = jax.random.fold_in(key, 7)
    first, second = jax.random.split(base, 2)
    width = HEADS * HD
    key_rows = jnp.clip(jax.random.normal(first, (TOKENS, width), jnp.float32), -4.0, 4.0)
    query_rows = jnp.clip(jax.random.normal(second, (TOKENS, width), jnp.float32), -4.0, 4.0)
    return (query_rows, key_rows)


def draw_queries(key, part):
    return paired_rows(key)[0].astype(jnp.bfloat16)


def draw_keys(key, part):
    return paired_rows(key)[1].astype(jnp.bfloat16)


def draw_levels(key, part):
    base = jax.random.fold_in(key, 11)
    groups = N_SEQ // 4
    scores = jax.random.randint(base, (groups, 4), 0, 1 << 20) * 4 + jnp.arange(4, dtype=jnp.int32)[None, :]
    order = jnp.argsort(scores, axis=1)
    table = jnp.array([2, 4, 4, 16], jnp.int32)
    return table[order].reshape(N_SEQ).astype(jnp.int32)


def block_scale(key, extent, pieces, low, top_value):
    loudness = 1.0
    for axis_at, parts in pieces:
        draws = jax.random.uniform(jax.random.fold_in(jax.random.fold_in(key, 6), axis_at), (parts,), jnp.float32, low / len(pieces), top_value / len(pieces))
        loudness = loudness * jnp.repeat(jnp.exp(draws), extent[axis_at] // parts).reshape((-1,) + (1,) * (len(extent) - 1 - axis_at))
    return loudness


def centred(stream_key, dims, scale, limit, cuts=(), kind=jnp.bfloat16):
    gain = block_scale(stream_key, dims, cuts, -0.22, 0.18) if cuts else 1.0
    values = jax.random.normal(stream_key, dims, jnp.float32) * scale * gain
    return jnp.minimum(jnp.maximum(values, -limit), limit).astype(kind)


def setup_inputs(seed: int = 0, part: int = 0) -> dict:
    splits = jax.random.split(jax.random.key(seed), 13)
    part_splits = jax.random.split(jax.random.fold_in(splits[12], part), 13)
    queries = draw_queries(jax.random.fold_in(jax.random.fold_in(splits[12], part), 71), part)
    keys = draw_keys(jax.random.fold_in(jax.random.fold_in(splits[12], part), 71), part)
    values = centred(part_splits[2], (TOKENS, HEADS * HD), 1.0, 6.0, ((0, 64),))
    history = centred(part_splits[3], (LATC, HPOS * N_SEQ), 1.0, 6.0, ((1, 64),))
    levels = draw_levels(jax.random.fold_in(jax.random.fold_in(splits[12], part), 71), part)
    patch_two = centred(splits[5], (2 * LATC, D), (2 * LATC) ** -0.5, 1.0)
    patch_four = centred(splits[6], (4 * LATC, D), (4 * LATC) ** -0.5, 0.75)
    patch_sixteen = centred(splits[7], (16 * LATC, D), (16 * LATC) ** -0.5, 0.375)
    mod_scale = jnp.clip(jax.random.uniform(splits[8], (D,), jnp.float32, -0.5, 0.5), -0.5, 0.5)
    mod_shift = centred(splits[9], (D,), 1.0, 4.0, (), jnp.float32)
    kv_weight = centred(splits[10], (D, 2 * HEADS * HD), D ** -0.5, 0.109375, ((1, 64),))
    key_gain = jnp.clip(jnp.exp(jax.random.uniform(splits[11], (HD,), jnp.float32, math.log(0.5), math.log(2.0))), 0.5, 2.0)
    return {"queries": queries, "keys": keys, "values": values, "history": history, "levels": levels, "patch_two": patch_two, "patch_four": patch_four, "patch_sixteen": patch_sixteen, "mod_scale": mod_scale, "mod_shift": mod_shift, "kv_weight": kv_weight, "key_gain": key_gain}


EPS = 1e-06

def level_tokens(history, weight, level):
    width = history.shape[1]
    grouped = history.reshape(LATC, width // level, level).transpose(1, 0, 2).reshape(width // level, LATC * level)
    return jnp.dot(grouped, weight, preferred_element_type=jnp.float32).astype(jnp.bfloat16)

def reference(queries, keys, values, history, levels, patch_two, patch_four, patch_sixteen, mod_scale, mod_shift, kv_weight, key_gain):
    counts = (HPOS // levels).astype(jnp.int32)
    ends = jnp.cumsum(counts).astype(jnp.int32)
    starts = ends - counts
    place = jnp.arange(HIST, dtype=jnp.int32)
    owner = lax.optimization_barrier(jnp.sum((ends[None, :] <= place[:, None]).astype(jnp.int32), axis=1)).astype(jnp.int32)
    inner = (place - starts[owner]).astype(jnp.int32)
    level = levels[owner]
    tokens_two = level_tokens(history, patch_two, 2)
    tokens_four = level_tokens(history, patch_four, 4)
    tokens_sixteen = level_tokens(history, patch_sixteen, 16)
    pick_two = jnp.take(tokens_two, (owner * (HPOS // 2) + jnp.minimum(inner, HPOS // 2 - 1)).astype(jnp.int32), axis=0)
    pick_four = jnp.take(tokens_four, (owner * (HPOS // 4) + jnp.minimum(inner, HPOS // 4 - 1)).astype(jnp.int32), axis=0)
    pick_sixteen = jnp.take(tokens_sixteen, (owner * (HPOS // 16) + jnp.minimum(inner, HPOS // 16 - 1)).astype(jnp.int32), axis=0)
    hidden = jnp.where((level == 2)[:, None], pick_two, jnp.where((level == 4)[:, None], pick_four, pick_sixteen))
    feats = hidden.astype(jnp.float32)
    mean = lax.optimization_barrier(jnp.mean(feats, axis=1, keepdims=True))
    centered = feats - mean
    var = lax.optimization_barrier(jnp.mean(centered * centered, axis=1, keepdims=True))
    normed = (centered * lax.rsqrt(var + EPS) * (1.0 + mod_scale) + mod_shift).astype(jnp.bfloat16)
    history_kv = jnp.dot(normed, kv_weight, preferred_element_type=jnp.float32).astype(jnp.bfloat16)
    pairs = history_kv.reshape(HIST, HD, 2, HEADS).transpose(0, 3, 2, 1)
    first = pairs[:, :, 0, :].astype(jnp.float32)
    history_keys = (first * lax.rsqrt(lax.optimization_barrier(jnp.mean(first * first, axis=-1, keepdims=True)) + EPS) * key_gain).astype(jnp.bfloat16)
    history_values = pairs[:, :, 1, :]
    scale = HD ** (-0.5)

    def one_head(item):
        query, key_part, value_part, hist_key, hist_value = item
        all_keys = jnp.concatenate([key_part, hist_key], axis=0)
        all_values = jnp.concatenate([value_part, hist_value], axis=0)
        scores = jnp.dot(query, all_keys.T, preferred_element_type=jnp.float32) * scale
        top = lax.optimization_barrier(jnp.max(scores, axis=1, keepdims=True))
        weights = jnp.exp(scores - top)
        total = lax.optimization_barrier(jnp.sum(weights, axis=1, keepdims=True))
        probs = weights.astype(jnp.bfloat16)
        mixed = jnp.dot(probs, all_values, preferred_element_type=jnp.float32) / total
        return mixed.astype(jnp.bfloat16)
    split_q = queries.reshape(TOKENS, HEADS, HD).transpose(1, 0, 2)
    split_k = keys.reshape(TOKENS, HEADS, HD).transpose(1, 0, 2)
    split_v = values.reshape(TOKENS, HEADS, HD).transpose(1, 0, 2)
    result = lax.map(one_head, (split_q, split_k, split_v, history_keys.transpose(1, 0, 2), history_values.transpose(1, 0, 2)))
    return result.transpose(1, 0, 2).reshape(TOKENS, HEADS * HD)
```

```python
import functools
import math

import jax
import jax.numpy as jnp
from jax import lax
from jax.experimental import pallas as pl
from jax.experimental.pallas import tpu as pltpu
from jax.sharding import PartitionSpec as P

EPS = 1e-06
BF = jnp.bfloat16
F32 = jnp.float32
LOW = -1e30


def device_of(head, part):
    z, pair = divmod(head, 2)
    side, core = divmod(part, 2)
    x = (0, 1, 3, 2)[pair * 2 + side]
    return z * 8 + x * 2 + core


HEAD_GROUPS = [[device_of(g, p) for g in range(16)] for p in range(4)]
CORE_SWAP = [(d, d ^ 1) for d in range(64)]
SIDE_SWAP = [(d, d ^ 2) for d in range(64)]


def to_heads(array):
    return lax.all_to_all(array, "seq", 0, 0, tiled=True, axis_index_groups=HEAD_GROUPS)


def dot_nt(a, b):
    return lax.dot_general(a, b, (((1,), (1,)), ((), ())), preferred_element_type=F32)


def dot_nn(a, b):
    return jnp.dot(a, b, preferred_element_type=F32)


def repeated(x, n):
    return x if n == 1 else jnp.concatenate([x] * n, axis=1)


def history_kernel(x2, x4, x16, p2, p4, p16, scale, shift, weight, out):
    gain = 1.0 + scale[...]
    bias = shift[...]

    def project(tokens, patch, rows):
        hidden = dot_nn(tokens, patch[...]).astype(BF).astype(F32)
        width = hidden.shape[1]
        mean = jnp.sum(hidden, axis=1, keepdims=True) * (1.0 / width)
        centered = hidden - mean
        var = jnp.sum(centered * centered, axis=1, keepdims=True) * (1.0 / width)
        normed = (centered * lax.rsqrt(var + EPS) * gain + bias).astype(BF)
        return lax.dot_general(
            weight[...], normed, (((0,), (1,)), ((), ())), preferred_element_type=F32
        ).astype(BF)

    for i in range(4):
        out[:, i * 128 : (i + 1) * 128] = project(x2[i * 128 : (i + 1) * 128, :], p2, 128)
    for i in range(4):
        out[:, 512 + i * 128 : 512 + (i + 1) * 128] = project(
            x4[i * 128 : (i + 1) * 128, :], p4, 128
        )
    last = project(x16[...], p16, 64)
    out[:, 1024:1152] = jnp.concatenate([last, jnp.zeros_like(last)], axis=1)


def history_share(x2, x4, x16, p2, p4, p16, scale, shift, weight):
    return pl.pallas_call(
        history_kernel,
        out_shape=jax.ShapeDtypeStruct((64, 1152), BF),
        compiler_params=pltpu.CompilerParams(vmem_limit_bytes=50 << 20),
        cost_estimate=pl.CostEstimate(
            flops=8_000_000_000, transcendentals=1088, bytes_accessed=3_000_000
        ),
    )(x2, x4, x16, p2, p4, p16, scale[None], shift[None], weight)


def attend_kernel(cfg, *refs):
    pairs, with_hist, first, last, scale, block = cfg
    refs = list(refs)
    q_ref = refs.pop(0)
    kv = [(refs.pop(0), refs.pop(0)) for _ in range(pairs)]
    if with_hist:
        hist_ref = refs.pop(0)
        gain_ref = refs.pop(0)
    if not first:
        top_in, total_in, acc_in = refs.pop(0), refs.pop(0), refs.pop(0)
    if last:
        out_ref = refs.pop(0)
    else:
        top_out, total_out, acc_out = refs.pop(0), refs.pop(0), refs.pop(0)
    if with_hist:
        hist_keys, hist_vals = refs.pop(0), refs.pop(0)

        @pl.when(pl.program_id(0) == 0)
        def _():
            raw = hist_ref[0].astype(F32)
            mean = jnp.sum(raw * raw, axis=0, keepdims=True) * (1.0 / 128)
            normed = (raw * lax.rsqrt(mean + EPS) * gain_ref[...]).astype(BF)
            hist_keys[0:128, :] = normed
            hist_keys[128:256, :] = normed
            hist_vals[0:128, :] = hist_ref[1]
            hist_vals[128:256, :] = jnp.ones((128, 1152), BF)

    q = q_ref[...].reshape(-1, 128)
    rows = q.shape[0]
    scaled = q.astype(F32) * scale
    high = scaled.astype(BF)
    low = (scaled - high.astype(F32)).astype(BF)
    q2 = jnp.concatenate([high, low], axis=1)
    if first:
        top = jnp.full((rows, 128), LOW, F32)
        total = jnp.zeros((rows, 128), F32)
        acc = jnp.zeros((rows, 128), F32)
    else:
        top, total, acc = top_in[0], total_in[0], acc_in[0]

    steps = []
    for k_ref, v_ref in kv:
        for i in range(1024 // block):
            steps.append(("section", k_ref, v_ref, i))
    if with_hist:
        steps.append(("history", 0, 1024, 0))
        steps.append(("history", 1024, 1152, 0))

    def scores(step):
        kind, a, b, i = step
        if kind == "section":
            keys = a[i * block // 64 : (i + 1) * block // 64].reshape(block, 128)
            return dot_nt(q2, jnp.concatenate([keys, keys], axis=1))
        s = dot_nn(q2, hist_keys[:, a:b])
        if b == 1152:
            s = jnp.where(lax.broadcasted_iota(jnp.int32, s.shape, 1) < 64, s, LOW)
        return s

    def mixed(step, probs):
        kind, a, b, i = step
        if kind == "section":
            vals = b[i * block // 64 : (i + 1) * block // 64].reshape(block, 128)
            return dot_nn(probs, jnp.concatenate([vals, jnp.ones_like(vals)], axis=1))
        return dot_nt(probs, hist_vals[:, a:b])

    ahead = scores(steps[0])
    for n, step in enumerate(steps):
        s = ahead
        if n + 1 < len(steps):
            ahead = scores(steps[n + 1])
        newer = jnp.maximum(top, jnp.max(s, axis=1, keepdims=True))
        probs = jnp.exp2(s - repeated(newer, s.shape[1] // 128)).astype(BF)
        fade = jnp.exp2(top - newer)
        part = mixed(step, probs)
        acc = acc * fade + part[:, :128]
        total = total * fade + part[:, 128:]
        top = newer
    if last:
        out_ref[...] = (acc / total).astype(BF).reshape(out_ref.shape)
    else:
        top_out[0] = top
        total_out[0] = total
        acc_out[0] = acc


def attend(q_array, kvs, state, hist, gain, half, scale, block=1024):
    first = state is None
    last = hist is not None
    tile = 8
    if half is None:
        grid = (4,)
        q_map = lambda i: (i % 2, i // 2, 0)
        s_map = lambda i: (i // 2, i % 2, 0)
    else:
        grid = (2,)
        q_map = lambda i: (i, half, 0)
        s_map = lambda i: (half, i, 0)
    state_spec = pl.BlockSpec((1, tile * 64, 128), s_map)
    args = [q_array]
    in_specs = [pl.BlockSpec((tile, 64, 128), q_map)]
    for array in kvs:
        args += [array, array]
        in_specs += [
            pl.BlockSpec((16, 64, 128), lambda i: (0, 0, 0)),
            pl.BlockSpec((16, 64, 128), lambda i: (0, 1, 0)),
        ]
    scratch = []
    n_keys = 1024 * len(kvs)
    if hist is not None:
        args += [hist, gain]
        in_specs += [
            pl.BlockSpec((2, 128, 1152), lambda i: (0, 0, 0)),
            pl.BlockSpec((128, 1), lambda i: (0, 0)),
        ]
        scratch = [pltpu.VMEM((256, 1152), BF), pltpu.VMEM((256, 1152), BF)]
        n_keys += 1152
    if not first:
        args += list(state)
        in_specs += [state_spec] * 3
    if last:
        out_shape = jax.ShapeDtypeStruct((16, 64, 128), BF)
        out_specs = pl.BlockSpec((tile, 64, 128), lambda i: (i, 0, 0))
    else:
        out_shape = [jax.ShapeDtypeStruct((2, 1024, 128), F32)] * 3
        out_specs = [state_spec] * 3
    n_rows = grid[0] * tile * 64
    return pl.pallas_call(
        functools.partial(
            attend_kernel, (len(kvs), hist is not None, first, last, scale, block)
        ),
        grid=grid,
        in_specs=in_specs,
        out_specs=out_specs,
        out_shape=out_shape,
        scratch_shapes=scratch,
        compiler_params=pltpu.CompilerParams(
            vmem_limit_bytes=56 << 20, dimension_semantics=("arbitrary",)
        ),
        cost_estimate=pl.CostEstimate(
            flops=8 * n_rows * n_keys * 128,
            transcendentals=n_rows * n_keys,
            bytes_accessed=n_keys * 512 + n_rows * 2048,
        ),
    )(*args)


def sorted_blocks(levels):
    table = levels.reshape(16, 4)
    fours = table == 4
    earlier = jnp.cumsum(fours.astype(jnp.int32), axis=1)
    kinds = jnp.stack(
        [table == 2, fours & (earlier == 1), fours & (earlier == 2), table == 16]
    )
    same = jnp.arange(16)[:, None] == jnp.arange(16)[None, :]
    return (kinds[:, :, None, :] & same[None, :, :, None]).reshape(64, 64).astype(BF)


def shards(
    queries,
    keys,
    values,
    history,
    levels,
    patch_two,
    patch_four,
    patch_sixteen,
    mod_scale,
    mod_shift,
    kv_weight,
    key_gain,
):
    scale = 128 ** (-0.5) * math.log2(math.e)
    q_heads = queries.reshape(128, 16, 128).transpose(1, 0, 2)
    k_heads = keys.reshape(128, 16, 128).transpose(1, 0, 2)
    v_heads = values.reshape(128, 16, 128).transpose(1, 0, 2)
    send_a = jnp.concatenate([q_heads, k_heads[:, :64], v_heads[:, :64]], axis=1)
    send_b = jnp.concatenate([k_heads[:, 64:], v_heads[:, 64:]], axis=1)

    mine = levels[lax.axis_index("seq")]

    def arranged(level):
        return history.reshape(16, 64 // level, level).transpose(1, 0, 2).reshape(8, 128)

    packed = jnp.where(
        mine == 2, arranged(2), jnp.where(mine == 4, arranged(4), arranged(16))
    )
    everything = lax.all_to_all(
        jnp.broadcast_to(packed[None], (64, 8, 128)), "seq", 0, 0, tiled=True
    ).reshape(64, 1024)
    got_a = to_heads(send_a)

    ordered = dot_nn(sorted_blocks(levels), everything).astype(BF)
    share = history_share(
        ordered[:16].reshape(512, 32),
        ordered[16:48].reshape(512, 64),
        ordered[48:].reshape(64, 256),
        patch_two,
        patch_four,
        patch_sixteen,
        mod_scale,
        mod_shift,
        kv_weight,
    )
    share = share.reshape(2, 2, 16, 1152).transpose(2, 1, 0, 3).reshape(16, 1, 4, 1152)
    share = jnp.broadcast_to(share, (16, 4, 4, 1152)).reshape(64, 4, 1152)
    got_hist = lax.all_to_all(share, "seq", 0, 0, tiled=True)
    got_b = to_heads(send_b)

    kv_a = got_a[:, 128:]
    core_a = lax.ppermute(kv_a, "seq", CORE_SWAP)
    side_a = lax.ppermute(kv_a, "seq", SIDE_SWAP)
    far_a = lax.ppermute(side_a, "seq", CORE_SWAP)
    core_b = lax.ppermute(got_b, "seq", CORE_SWAP)
    side_b = lax.ppermute(got_b, "seq", SIDE_SWAP)
    far_b = lax.ppermute(side_b, "seq", CORE_SWAP)
    hist = got_hist.reshape(64, 2, 2, 1152).transpose(1, 0, 2, 3).reshape(2, 128, 1152)
    gain = key_gain[:, None]

    state = attend(got_a, [kv_a, core_a], None, None, None, None, scale)
    state = attend(got_a, [side_a, far_a], state, None, None, None, scale)
    state = attend(got_a, [got_b, core_b], state, None, None, None, scale)
    outs = []
    for half in range(2):
        mixed = attend(got_a, [side_b, far_b], state, hist, gain, half, scale)
        outs.append(to_heads(mixed))
    out = jnp.concatenate(outs, axis=1)
    return out.transpose(1, 0, 2).reshape(128, 2048)


def solution(mesh):
    return jax.shard_map(
        shards,
        mesh=mesh,
        in_specs=(
            P(("video", "seq"), None),
            P(("video", "seq"), None),
            P(("video", "seq"), None),
            P(None, ("video", "seq")),
            P("video"),
            P(),
            P(),
            P(),
            P(),
            P(),
            P(None, "seq"),
            P(),
        ),
        out_specs=P(("video", "seq"), None),
        check_vma=False,
    )
```

```python
import functools
import math

import jax
import jax.numpy as jnp
from jax import lax
from jax.experimental import pallas as pl
from jax.experimental.pallas import tpu as pltpu
from jax.sharding import PartitionSpec as P

EPS = 1e-06
BF = jnp.bfloat16
F32 = jnp.float32
LOW = -1e30
VL = 56


def device_of(head, part):
    z, pair = divmod(head, 2)
    side, core = divmod(part, 2)
    x = (0, 1, 3, 2)[pair * 2 + side]
    return z * 8 + x * 2 + core


HEAD_GROUPS = [[device_of(g, p) for g in range(16)] for p in range(4)]
CORE_SWAP = [(d, d ^ 1) for d in range(64)]
SIDE_SWAP = [(d, d ^ 2) for d in range(64)]


def to_heads(array):
    return lax.all_to_all(array, "seq", 0, 0, tiled=True, axis_index_groups=HEAD_GROUPS)


def dot_nt(a, b):
    return lax.dot_general(a, b, (((1,), (1,)), ((), ())), preferred_element_type=F32)


def dot_nn(a, b):
    return jnp.dot(a, b, preferred_element_type=F32)


def repeated(x, n):
    return x if n == 1 else jnp.concatenate([x] * n, axis=1)


def pack_kernel(levels, mine, q, k, v, history, out, packed):
    @pl.when(pl.program_id(0) == 0)
    def _():
        level = levels[mine[0]]
        lane_channel = lax.broadcasted_iota(jnp.int32, (16, 128), 1) % 16
        spread = (lane_channel == lax.broadcasted_iota(jnp.int32, (16, 128), 0)).astype(BF)
        tiled = lax.dot_general(
            history[...], spread, (((0,), (0,)), ((), ())), preferred_element_type=F32
        )

        def row_and_piece(pos):
            row = jnp.where(
                level == 2,
                pos % 16 // 2,
                jnp.where(level == 4, pos % 32 // 4, pos % 16 // 8 * 4 + pos // 16),
            )
            piece = jnp.where(
                level == 2,
                pos // 16 * 2 + pos % 2,
                jnp.where(level == 4, pos // 32 * 4 + pos % 4, pos % 8),
            )
            return row, piece

        _, piece = row_and_piece(lax.broadcasted_iota(jnp.int32, (64, 128), 0))
        lane_piece = lax.broadcasted_iota(jnp.int32, (64, 128), 1) // 16
        kept = jnp.where(piece == lane_piece, tiled, 0.0).astype(BF)
        row, _ = row_and_piece(lax.broadcasted_iota(jnp.int32, (8, 64), 1))
        pick = (row == lax.broadcasted_iota(jnp.int32, (8, 64), 0)).astype(BF)
        packed[...] = dot_nn(pick, kept).astype(BF)

    for h in range(4):
        cols = slice(h * 128, (h + 1) * 128)
        out[h, 0:128, :] = q[:, cols]
        out[h, 128:256, :] = k[:, cols]
        out[h, 256:384, :] = v[:, cols]
        out[h, 384:392, :] = packed[...]


def pack(levels, mine, queries, keys, values, history):
    spec = pl.BlockSpec((128, 512), lambda i, *_: (0, i))
    return pl.pallas_call(
        pack_kernel,
        grid_spec=pltpu.PrefetchScalarGridSpec(
            num_scalar_prefetch=2,
            grid=(4,),
            in_specs=[spec, spec, spec, pl.BlockSpec((16, 64), lambda i, *_: (0, 0))],
            out_specs=pl.BlockSpec((4, 392, 128), lambda i, *_: (i, 0, 0)),
            scratch_shapes=[pltpu.VMEM((8, 128), BF)],
        ),
        out_shape=jax.ShapeDtypeStruct((16, 392, 128), BF),
        compiler_params=pltpu.CompilerParams(dimension_semantics=("arbitrary",)),
    )(levels, mine, queries, keys, values, history)


def history_kernel(heard, rank, patches, scale, shift, weight, out):
    raw = heard[...].reshape(512, 128)
    place = lax.broadcasted_iota(jnp.int32, (512, 512), 0) == rank[...]
    tokens = dot_nn(place.astype(BF), raw).astype(BF)
    gain = 1.0 + scale[...]
    bias = shift[...]
    lane = lax.broadcasted_iota(jnp.int32, (128, 128), 1)

    def finish(total, slot):
        hidden = total.astype(BF).astype(F32)
        width = hidden.shape[1]
        mean = jnp.sum(hidden, axis=1, keepdims=True) * (1.0 / width)
        centered = hidden - mean
        var = jnp.sum(centered * centered, axis=1, keepdims=True) * (1.0 / width)
        normed = (centered * lax.rsqrt(var + EPS) * gain + bias).astype(BF)
        out[:, slot * 128 : (slot + 1) * 128] = lax.dot_general(
            weight[...], normed, (((0,), (1,)), ((), ())), preferred_element_type=F32
        ).astype(BF)

    def part(first, lanes, index):
        block = tokens[first : first + 128, :]
        return jnp.where(lane // lanes == index, block, jnp.zeros_like(block))

    for i in range(4):
        finish(dot_nn(part(0, 32, i), patches[0:128, :]), i)
    for i in range(4):
        finish(dot_nn(part(128 + 128 * (i // 2), 64, i % 2), patches[128:256, :]), 4 + i)
    block = tokens[384:512, :]
    early = dot_nn(block, patches[256:384, :])
    late = dot_nn(block, patches[384:512, :])
    late = jnp.concatenate([late[4:], late[:4]], axis=0)
    finish(early + late, 8)


def history_share(heard, rank, patches, scale, shift, weight):
    full = lambda *shape: pl.BlockSpec(shape, lambda i: (0,) * len(shape))
    return pl.pallas_call(
        history_kernel,
        grid=(1,),
        in_specs=[
            full(4, 16, 8, 128),
            full(1, 512),
            full(512, 3072),
            full(1, 3072),
            full(1, 3072),
            full(3072, 64),
        ],
        out_specs=full(64, 1152),
        out_shape=jax.ShapeDtypeStruct((64, 1152), BF),
        compiler_params=pltpu.CompilerParams(vmem_limit_bytes=40 << 20),
        cost_estimate=pl.CostEstimate(
            flops=8_000_000_000, transcendentals=1152, bytes_accessed=4_000_000
        ),
    )(heard, rank, patches, scale[None], shift[None], weight)


def attend_kernel(cfg, *refs):
    pairs, with_hist, first, last, scale, block = cfg
    refs = list(refs)
    q_ref = refs.pop(0)
    kv = [(refs.pop(0), refs.pop(0)) for _ in range(pairs)]
    if with_hist:
        hist_ref = refs.pop(0)
        gain_ref = refs.pop(0)
    if not first:
        stats_in, acc_in = refs.pop(0), refs.pop(0)
    if last:
        out_ref = refs.pop(0)
    else:
        stats_out, acc_out = refs.pop(0), refs.pop(0)
    if with_hist:
        hist_keys, hist_vals = refs.pop(0), refs.pop(0)

        @pl.when(pl.program_id(0) == 0)
        def _():
            row = lax.broadcasted_iota(jnp.int32, (256, 256), 0)
            col = lax.broadcasted_iota(jnp.int32, (256, 256), 1)
            source = row % 128 // 2 * 4 + row // 128 * 2 + row % 2
            raw = dot_nn((source == col).astype(BF), hist_ref[...])
            keys = raw[0:128, :]
            mean = jnp.sum(keys * keys, axis=0, keepdims=True) * (1.0 / 128)
            normed = (keys * lax.rsqrt(mean + EPS) * gain_ref[...]).astype(BF)
            hist_keys[0:128, :] = normed
            hist_keys[128:256, :] = normed
            hist_vals[0:128, :] = raw[128:256, :].astype(BF)
            hist_vals[128:256, :] = jnp.ones((128, 1152), BF)

    q = q_ref[...].reshape(-1, 128)
    rows = q.shape[0]
    scaled = q.astype(F32) * scale
    high = scaled.astype(BF)
    low = (scaled - high.astype(F32)).astype(BF)
    q2 = jnp.concatenate([high, low], axis=1)
    if first:
        top = jnp.full((rows, 128), LOW, F32)
        total = jnp.zeros((rows, 128), F32)
        acc = jnp.zeros((rows, 128), F32)
    else:
        stats = stats_in[...]
        top = jnp.broadcast_to(stats[:, 0:1], (rows, 128))
        total = jnp.broadcast_to(stats[:, 127:128], (rows, 128))
        acc = acc_in[...]

    steps = []
    for k_ref, v_ref in kv:
        for i in range(2048 // block):
            steps.append(("section", k_ref, v_ref, i))
    if with_hist:
        steps.append(("history", 0, 1024, 0))
        steps.append(("history", 1024, 1152, 0))

    def scores(step):
        kind, a, b, i = step
        if kind == "section":
            keys = a[i * block // 128 : (i + 1) * block // 128].reshape(block, 128)
            return dot_nt(q2, jnp.concatenate([keys, keys], axis=1))
        s = dot_nn(q2, hist_keys[:, a:b])
        if b == 1152:
            s = jnp.where(lax.broadcasted_iota(jnp.int32, s.shape, 1) % 8 < 4, s, LOW)
        return s

    def mixed(step, probs):
        kind, a, b, i = step
        if kind == "section":
            vals = b[i * block // 128 : (i + 1) * block // 128].reshape(block, 128)
            return dot_nn(probs, jnp.concatenate([vals, jnp.ones_like(vals)], axis=1))
        return dot_nt(probs, hist_vals[:, a:b])

    ahead = scores(steps[0])
    for n, step in enumerate(steps):
        s = ahead
        if n + 1 < len(steps):
            ahead = scores(steps[n + 1])
        newer = jnp.maximum(top, jnp.max(s, axis=1, keepdims=True))
        probs = jnp.exp2(s - repeated(newer, s.shape[1] // 128)).astype(BF)
        fade = jnp.exp2(top - newer)
        part = mixed(step, probs)
        acc = acc * fade + part[:, :128]
        total = total * fade + part[:, 128:]
        top = newer
    if last:
        out_ref[...] = (acc / total).astype(BF).reshape(out_ref.shape)
    else:
        low_lanes = lax.broadcasted_iota(jnp.int32, (rows, 128), 1) < 64
        stats_out[...] = jnp.where(low_lanes, top, total)
        acc_out[...] = acc


def attend(q_array, kvs, state, hist, gain, scale, block=1024):
    first = state is None
    last = hist is not None
    tile = 4
    rows = tile * 128
    q_map = lambda i: (i, 0, 0)
    state_spec = pl.BlockSpec((rows, 128), lambda i: (i, 0))
    args = [q_array]
    in_specs = [pl.BlockSpec((tile, 128, 128), q_map)]
    for array in kvs:
        args += [array, array]
        in_specs += [
            pl.BlockSpec((16, 128, 128), lambda i: (0, 0, 0)),
            pl.BlockSpec((16, 128, 128), lambda i: (0, 1, 0)),
        ]
    scratch = []
    n_keys = 2048 * len(kvs)
    if last:
        args += [hist, gain]
        in_specs += [
            pl.BlockSpec((256, 1152), lambda i: (0, 0)),
            pl.BlockSpec((128, 1), lambda i: (0, 0)),
        ]
        scratch = [pltpu.VMEM((256, 1152), BF), pltpu.VMEM((256, 1152), BF)]
        n_keys += 1152
    if not first:
        args += list(state)
        in_specs += [state_spec] * 2
    if last:
        out_shape = jax.ShapeDtypeStruct((16, 128, 128), BF)
        out_specs = pl.BlockSpec((tile, 128, 128), q_map)
    else:
        out_shape = [jax.ShapeDtypeStruct((2048, 128), F32)] * 2
        out_specs = [state_spec] * 2
    return pl.pallas_call(
        functools.partial(
            attend_kernel, (len(kvs), hist is not None, first, last, scale, block)
        ),
        grid=(16 // tile,),
        in_specs=in_specs,
        out_specs=out_specs,
        out_shape=out_shape,
        scratch_shapes=scratch,
        compiler_params=pltpu.CompilerParams(
            vmem_limit_bytes=VL << 20, dimension_semantics=("arbitrary",)
        ),
        cost_estimate=pl.CostEstimate(
            flops=8 * 2048 * n_keys * 128,
            transcendentals=2048 * n_keys,
            bytes_accessed=n_keys * 512 + 2048 * 2048,
        ),
    )(*args)


def arrival_rank(levels, mine):
    table = levels.reshape(16, 4)
    fours = table == 4
    second = (jnp.cumsum(fours.astype(jnp.int32), axis=1) == 2).astype(jnp.int32)
    kind = jnp.where(table == 2, 0, jnp.where(fours, 1 + second, 3))
    rank = (kind * 16 + jnp.arange(16, dtype=jnp.int32)[:, None]).reshape(64)
    x = mine % 8 // 2
    part = 2 * ((x == 1) | (x == 2)).astype(jnp.int32) + mine % 2
    first = jnp.array(HEAD_GROUPS, jnp.int32)[part]
    ids = (first[None, :] ^ jnp.arange(4, dtype=jnp.int32)[:, None]).reshape(64)
    same = ids[:, None] == jnp.arange(64, dtype=jnp.int32)[None, :]
    arrived = jnp.sum(jnp.where(same, rank[None, :], 0), axis=1)
    return (arrived[:, None] * 8 + jnp.arange(8, dtype=jnp.int32)[None, :]).reshape(1, 512)


def expanded_patches(patch_two, patch_four, patch_sixteen):
    def by_offset(patch, factor):
        return patch.reshape(16, factor, -1).transpose(1, 0, 2).reshape(16 * factor, -1)

    two = by_offset(patch_two, 2)
    four = by_offset(patch_four, 4)
    return jnp.concatenate([two] * 4 + [four] * 2 + [by_offset(patch_sixteen, 16)], axis=0)


def head_columns(weight):
    col = jnp.arange(64, dtype=jnp.int32)
    source = col % 2 * 32 + col // 2 % 2 * 16 + col // 4
    return dot_nn(weight, (col[:, None] == source[None, :]).astype(BF)).astype(BF)


def shards(
    queries,
    keys,
    values,
    history,
    levels,
    patch_two,
    patch_four,
    patch_sixteen,
    mod_scale,
    mod_shift,
    kv_weight,
    key_gain,
):
    scale = 128 ** (-0.5) * math.log2(math.e)
    mine = lax.axis_index("seq")
    send = pack(levels, mine[None].astype(jnp.int32), queries, keys, values, history)
    rank, patches, weight, gain, got = lax.optimization_barrier(
        (
            arrival_rank(levels, mine),
            expanded_patches(patch_two, patch_four, patch_sixteen),
            head_columns(kv_weight),
            key_gain[:, None],
            to_heads(send),
        )
    )
    heard = got[:, 384:]
    heard = jnp.stack([heard, lax.ppermute(heard, "seq", CORE_SWAP)])
    heard = jnp.concatenate([heard, lax.ppermute(heard, "seq", SIDE_SWAP)])
    heard, own = lax.optimization_barrier((heard, got[:, 128:384]))
    core = lax.ppermute(own, "seq", CORE_SWAP)
    side = lax.ppermute(own, "seq", SIDE_SWAP)
    share = history_share(heard, rank, patches, mod_scale, mod_shift, weight)
    share = jnp.broadcast_to(share.reshape(16, 1, 4, 1152), (16, 4, 4, 1152))
    share, got, own, core = lax.optimization_barrier((share.reshape(64, 4, 1152), got, own, core))
    got_hist = lax.all_to_all(share, "seq", 0, 0, tiled=True)
    state = attend(got, [own, core], None, None, None, scale)
    side, state = lax.optimization_barrier((side, state))
    far = lax.ppermute(side, "seq", CORE_SWAP)
    hist = got_hist.reshape(256, 1152)
    mixed = attend(got, [side, far], state, hist, gain, scale)
    return to_heads(mixed).transpose(1, 0, 2).reshape(128, 2048)


def solution(mesh):
    return jax.shard_map(
        shards,
        mesh=mesh,
        in_specs=(
            P(("video", "seq"), None),
            P(("video", "seq"), None),
            P(("video", "seq"), None),
            P(None, ("video", "seq")),
            P("video"),
            P(),
            P(),
            P(),
            P(),
            P(),
            P(None, "seq"),
            P(),
        ),
        out_specs=P(("video", "seq"), None),
        check_vma=False,
    )
```

```python
import functools
import math

import jax
import jax.numpy as jnp
from jax import lax
from jax.experimental import pallas as pl
from jax.experimental.pallas import tpu as pltpu
from jax.sharding import PartitionSpec as P

EPS = 1e-06
BF = jnp.bfloat16
F32 = jnp.float32
LOW = -1e30
VL = 56


def device_of(head, part):
    z, pair = divmod(head, 2)
    side, core = divmod(part, 2)
    x = (0, 1, 3, 2)[pair * 2 + side]
    return z * 8 + x * 2 + core


HEAD_GROUPS = [[device_of(g, p) for g in range(16)] for p in range(4)]
CORE_SWAP = [(d, d ^ 1) for d in range(64)]
SIDE_SWAP = [(d, d ^ 2) for d in range(64)]
BOTH_SWAP = [(d, d ^ 3) for d in range(64)]


def to_heads(array):
    return lax.all_to_all(array, "seq", 0, 0, tiled=True, axis_index_groups=HEAD_GROUPS)


def dot_nt(a, b):
    return lax.dot_general(a, b, (((1,), (1,)), ((), ())), preferred_element_type=F32)


def dot_nn(a, b):
    return jnp.dot(a, b, preferred_element_type=F32)


def repeated(x, n):
    return x if n == 1 else jnp.concatenate([x] * n, axis=1)


def pack_kernel(levels, mine, q, k, v, history, out, packed, sems):
    copies = []
    for part, array in enumerate((q, k, v)):
        for h in range(16):
            copies.append(
                pltpu.make_async_copy(
                    array.at[:, h * 128 : (h + 1) * 128],
                    out.at[h, part * 128 : (part + 1) * 128, :],
                    sems.at[part * 16 + h],
                )
            )
    for copy in copies:
        copy.start()

    level = levels[mine[0]]
    lane_channel = lax.broadcasted_iota(jnp.int32, (16, 128), 1) % 16
    spread = (lane_channel == lax.broadcasted_iota(jnp.int32, (16, 128), 0)).astype(BF)
    tiled = lax.dot_general(
        history[...], spread, (((0,), (0,)), ((), ())), preferred_element_type=F32
    )

    def row_and_piece(pos):
        row = jnp.where(
            level == 2,
            pos % 16 // 2,
            jnp.where(level == 4, pos % 32 // 4, pos % 16 // 8 * 4 + pos // 16),
        )
        piece = jnp.where(
            level == 2,
            pos // 16 * 2 + pos % 2,
            jnp.where(level == 4, pos // 32 * 4 + pos % 4, pos % 8),
        )
        return row, piece

    _, piece = row_and_piece(lax.broadcasted_iota(jnp.int32, (64, 128), 0))
    lane_piece = lax.broadcasted_iota(jnp.int32, (64, 128), 1) // 16
    kept = jnp.where(piece == lane_piece, tiled, 0.0).astype(BF)
    row, _ = row_and_piece(lax.broadcasted_iota(jnp.int32, (8, 64), 1))
    pick = (row == lax.broadcasted_iota(jnp.int32, (8, 64), 0)).astype(BF)
    rows = dot_nn(pick, kept).astype(BF)
    packed[...] = jnp.broadcast_to(rows[None], (16, 8, 128))
    last = pltpu.make_async_copy(packed, out.at[:, 384:392, :], sems.at[48])
    last.start()
    for copy in copies:
        copy.wait()
    last.wait()


def pack(levels, mine, queries, keys, values, history):
    far = pl.BlockSpec(memory_space=pltpu.HBM)
    return pl.pallas_call(
        pack_kernel,
        grid_spec=pltpu.PrefetchScalarGridSpec(
            num_scalar_prefetch=2,
            grid=(1,),
            in_specs=[far, far, far, pl.BlockSpec((16, 64), lambda i, *_: (0, 0))],
            out_specs=far,
            scratch_shapes=[pltpu.VMEM((16, 8, 128), BF), pltpu.SemaphoreType.DMA((49,))],
        ),
        out_shape=jax.ShapeDtypeStruct((16, 392, 128), BF),
        compiler_params=pltpu.CompilerParams(vmem_limit_bytes=8 << 20),
    )(levels, mine, queries, keys, values, history)


def history_kernel(heard, rank, patches_far, scale, shift, weight, out, patches, sems):
    fetches = []
    for i, (first, stop) in enumerate(((0, 128), (128, 256), (256, 512))):
        fetches.append(
            pltpu.make_async_copy(
                patches_far.at[first:stop, :], patches.at[first:stop, :], sems.at[i]
            )
        )
        fetches[i].start()
    raw = heard[...].reshape(512, 128)
    place = lax.broadcasted_iota(jnp.int32, (512, 512), 0) == rank[...]
    tokens = dot_nn(place.astype(BF), raw).astype(BF)
    gain = 1.0 + scale[...]
    bias = shift[...]
    lane = lax.broadcasted_iota(jnp.int32, (128, 128), 1)

    def finish(total, slot):
        hidden = total.astype(BF).astype(F32)
        width = hidden.shape[1]
        mean = jnp.sum(hidden, axis=1, keepdims=True) * (1.0 / width)
        centered = hidden - mean
        var = jnp.sum(centered * centered, axis=1, keepdims=True) * (1.0 / width)
        normed = (centered * lax.rsqrt(var + EPS) * gain + bias).astype(BF)
        share = dot_nn(normed, weight[...])
        out[:, slot * 128 : (slot + 1) * 128] = share.T.astype(BF)

    def part(first, lanes, index):
        block = tokens[first : first + 128, :]
        return jnp.where(lane // lanes == index, block, jnp.zeros_like(block))

    fetches[0].wait()
    for i in range(4):
        finish(dot_nn(part(0, 32, i), patches[0:128, :]), i)
    fetches[1].wait()
    for i in range(4):
        finish(dot_nn(part(128 + 128 * (i // 2), 64, i % 2), patches[128:256, :]), 4 + i)
    fetches[2].wait()
    block = tokens[384:512, :]
    early = dot_nn(block, patches[256:384, :])
    late = dot_nn(block, patches[384:512, :])
    late = jnp.concatenate([late[4:], late[:4]], axis=0)
    finish(early + late, 8)


def history_share(heard, rank, patches, scale, shift, weight):
    full = lambda *shape: pl.BlockSpec(shape, lambda i: (0,) * len(shape))
    return pl.pallas_call(
        history_kernel,
        grid=(1,),
        in_specs=[
            full(4, 16, 8, 128),
            full(1, 512),
            pl.BlockSpec(memory_space=pltpu.HBM),
            full(1, 3072),
            full(1, 3072),
            full(3072, 64),
        ],
        out_specs=full(64, 1152),
        out_shape=jax.ShapeDtypeStruct((64, 1152), BF),
        scratch_shapes=[pltpu.VMEM((512, 3072), BF), pltpu.SemaphoreType.DMA((3,))],
        compiler_params=pltpu.CompilerParams(vmem_limit_bytes=40 << 20),
        cost_estimate=pl.CostEstimate(
            flops=8_000_000_000, transcendentals=1152, bytes_accessed=4_000_000
        ),
    )(heard, rank, patches, scale[None], shift[None], weight)


def attend_kernel(cfg, *refs):
    pairs, with_hist, first, last, scale, block = cfg
    refs = list(refs)
    q_ref = refs.pop(0)
    kv = [(refs.pop(0), refs.pop(0)) for _ in range(pairs)]
    if with_hist:
        hist_ref = refs.pop(0)
        gain_ref = refs.pop(0)
    if not first:
        stats_in, acc_in = refs.pop(0), refs.pop(0)
    if last:
        out_ref = refs.pop(0)
    else:
        stats_out, acc_out = refs.pop(0), refs.pop(0)
    if with_hist:
        hist_keys, hist_vals = refs.pop(0), refs.pop(0)

        @pl.when(pl.program_id(0) == 0)
        def _():
            row = lax.broadcasted_iota(jnp.int32, (256, 256), 0)
            col = lax.broadcasted_iota(jnp.int32, (256, 256), 1)
            source = row % 128 // 2 * 4 + row // 128 * 2 + row % 2
            raw = dot_nn((source == col).astype(BF), hist_ref[...])
            keys = raw[0:128, :]
            mean = jnp.sum(keys * keys, axis=0, keepdims=True) * (1.0 / 128)
            gain = jnp.broadcast_to(gain_ref[...], (128, 128)).T[:, 0:1]
            normed = (keys * lax.rsqrt(mean + EPS) * gain).astype(BF)
            hist_keys[0:128, :] = normed
            hist_keys[128:256, :] = normed
            hist_vals[0:128, :] = raw[128:256, :].astype(BF)
            hist_vals[128:256, :] = jnp.ones((128, 1152), BF)

    q = q_ref[...].reshape(-1, 128)
    rows = q.shape[0]
    scaled = q.astype(F32) * scale
    high = scaled.astype(BF)
    low = (scaled - high.astype(F32)).astype(BF)
    q2 = jnp.concatenate([high, low], axis=1)
    if first:
        top = jnp.full((rows, 128), LOW, F32)
        total = jnp.zeros((rows, 128), F32)
        acc = jnp.zeros((rows, 128), F32)
    else:
        stats = stats_in[...]
        top = jnp.broadcast_to(stats[:, 0:1], (rows, 128))
        total = jnp.broadcast_to(stats[:, 127:128], (rows, 128))
        acc = acc_in[...]

    steps = []
    for k_ref, v_ref in kv:
        for i in range(2048 // block):
            steps.append(("section", k_ref, v_ref, i))
    if with_hist:
        steps.append(("history", 0, 1024, 0))
        steps.append(("history", 1024, 1152, 0))

    def scores(step):
        kind, a, b, i = step
        if kind == "section":
            keys = a[i * block // 128 : (i + 1) * block // 128].reshape(block, 128)
            return dot_nt(q2, jnp.concatenate([keys, keys], axis=1))
        s = dot_nn(q2, hist_keys[:, a:b])
        if b == 1152:
            s = jnp.where(lax.broadcasted_iota(jnp.int32, s.shape, 1) % 8 < 4, s, LOW)
        return s

    def mixed(step, probs):
        kind, a, b, i = step
        if kind == "section":
            vals = b[i * block // 128 : (i + 1) * block // 128].reshape(block, 128)
            return dot_nn(probs, jnp.concatenate([vals, jnp.ones_like(vals)], axis=1))
        return dot_nt(probs, hist_vals[:, a:b])

    ahead = scores(steps[0])
    for n, step in enumerate(steps):
        s = ahead
        if n + 1 < len(steps):
            ahead = scores(steps[n + 1])
        newer = jnp.maximum(top, jnp.max(s, axis=1, keepdims=True))
        probs = jnp.exp2(s - repeated(newer, s.shape[1] // 128)).astype(BF)
        fade = jnp.exp2(top - newer)
        part = mixed(step, probs)
        acc = acc * fade + part[:, :128]
        total = total * fade + part[:, 128:]
        top = newer
    if last:
        out_ref[...] = (acc / total).astype(BF).reshape(out_ref.shape)
    else:
        low_lanes = lax.broadcasted_iota(jnp.int32, (rows, 128), 1) < 64
        stats_out[...] = jnp.where(low_lanes, top, total)
        acc_out[...] = acc


def attend(q_array, kvs, state, hist, gain, scale, block=1024):
    first = state is None
    last = hist is not None
    tile = 4
    rows = tile * 128
    q_map = lambda i: (i, 0, 0)
    state_spec = pl.BlockSpec((rows, 128), lambda i: (i, 0))
    args = [q_array]
    in_specs = [pl.BlockSpec((tile, 128, 128), q_map)]
    for array in kvs:
        args += [array, array]
        in_specs += [
            pl.BlockSpec((16, 128, 128), lambda i: (0, 0, 0)),
            pl.BlockSpec((16, 128, 128), lambda i: (0, 1, 0)),
        ]
    scratch = []
    n_keys = 2048 * len(kvs)
    if last:
        args += [hist, gain]
        in_specs += [
            pl.BlockSpec((256, 1152), lambda i: (0, 0)),
            pl.BlockSpec((1, 128), lambda i: (0, 0)),
        ]
        scratch = [pltpu.VMEM((256, 1152), BF), pltpu.VMEM((256, 1152), BF)]
        n_keys += 1152
    if not first:
        args += list(state)
        in_specs += [state_spec] * 2
    if last:
        out_shape = jax.ShapeDtypeStruct((16, 128, 128), BF)
        out_specs = pl.BlockSpec((tile, 128, 128), q_map)
    else:
        out_shape = [jax.ShapeDtypeStruct((2048, 128), F32)] * 2
        out_specs = [state_spec] * 2
    return pl.pallas_call(
        functools.partial(
            attend_kernel, (len(kvs), hist is not None, first, last, scale, block)
        ),
        grid=(16 // tile,),
        in_specs=in_specs,
        out_specs=out_specs,
        out_shape=out_shape,
        scratch_shapes=scratch,
        compiler_params=pltpu.CompilerParams(
            vmem_limit_bytes=VL << 20, dimension_semantics=("arbitrary",)
        ),
        cost_estimate=pl.CostEstimate(
            flops=8 * 2048 * n_keys * 128,
            transcendentals=2048 * n_keys,
            bytes_accessed=n_keys * 512 + 2048 * 2048,
        ),
    )(*args)


def arrival_rank(levels, mine):
    table = levels.reshape(16, 4)
    fours = table == 4
    second = (jnp.cumsum(fours.astype(jnp.int32), axis=1) == 2).astype(jnp.int32)
    kind = jnp.where(table == 2, 0, jnp.where(fours, 1 + second, 3))
    rank = (kind * 16 + jnp.arange(16, dtype=jnp.int32)[:, None]).reshape(64)
    x = mine % 8 // 2
    part = 2 * ((x == 1) | (x == 2)).astype(jnp.int32) + mine % 2
    first = jnp.array(HEAD_GROUPS, jnp.int32)[part]
    ids = (first[None, :] ^ jnp.arange(4, dtype=jnp.int32)[:, None]).reshape(64)
    same = ids[:, None] == jnp.arange(64, dtype=jnp.int32)[None, :]
    arrived = jnp.sum(jnp.where(same, rank[None, :], 0), axis=1)
    return (arrived[:, None] * 8 + jnp.arange(8, dtype=jnp.int32)[None, :]).reshape(1, 512)


def expanded_patches(patch_two, patch_four, patch_sixteen):
    def by_offset(patch, factor):
        return patch.reshape(16, factor, -1).transpose(1, 0, 2).reshape(16 * factor, -1)

    two = by_offset(patch_two, 2)
    four = by_offset(patch_four, 4)
    return jnp.concatenate([two] * 4 + [four] * 2 + [by_offset(patch_sixteen, 16)], axis=0)


def head_columns(weight):
    col = jnp.arange(64, dtype=jnp.int32)
    source = col % 2 * 32 + col // 2 % 2 * 16 + col // 4
    return dot_nn(weight, (col[:, None] == source[None, :]).astype(BF)).astype(BF)


def shards(
    queries,
    keys,
    values,
    history,
    levels,
    patch_two,
    patch_four,
    patch_sixteen,
    mod_scale,
    mod_shift,
    kv_weight,
    key_gain,
):
    scale = 128 ** (-0.5) * math.log2(math.e)
    mine = lax.axis_index("seq")
    send = pack(levels, mine[None].astype(jnp.int32), queries, keys, values, history)
    rank, patches, weight, got = lax.optimization_barrier(
        (
            arrival_rank(levels, mine),
            expanded_patches(patch_two, patch_four, patch_sixteen),
            head_columns(kv_weight),
            to_heads(send),
        )
    )
    heard = got[:, 384:]
    near = lax.ppermute(heard, "seq", CORE_SWAP)
    across = lax.ppermute(heard, "seq", SIDE_SWAP)
    beyond = lax.ppermute(heard, "seq", BOTH_SWAP)
    near, own = lax.optimization_barrier((near, got[:, 128:384]))
    heard = jnp.stack([heard, near, across, beyond])
    core = lax.ppermute(own, "seq", CORE_SWAP)
    side = lax.ppermute(own, "seq", SIDE_SWAP)
    share = history_share(heard, rank, patches, mod_scale, mod_shift, weight)
    share = jnp.broadcast_to(share.reshape(16, 1, 4, 1152), (16, 4, 4, 1152))
    share, got, own, core = lax.optimization_barrier((share.reshape(64, 4, 1152), got, own, core))
    got_hist = lax.all_to_all(share, "seq", 0, 0, tiled=True)
    state = attend(got, [own, core], None, None, None, scale)
    side, state = lax.optimization_barrier((side, state))
    far = lax.ppermute(side, "seq", CORE_SWAP)
    hist = got_hist.reshape(256, 1152)
    mixed = attend(got, [side, far], state, hist, key_gain[None], scale)
    return to_heads(mixed).transpose(1, 0, 2).reshape(128, 2048)


def solution(mesh):
    return jax.shard_map(
        shards,
        mesh=mesh,
        in_specs=(
            P(("video", "seq"), None),
            P(("video", "seq"), None),
            P(("video", "seq"), None),
            P(None, ("video", "seq")),
            P("video"),
            P(),
            P(),
            P(),
            P(),
            P(),
            P(None, "seq"),
            P(),
        ),
        out_specs=P(("video", "seq"), None),
        check_vma=False,
    )
```

```python
import functools
import math

import jax
import jax.numpy as jnp
from jax import lax
from jax.experimental import pallas as pl
from jax.experimental.pallas import tpu as pltpu
from jax.sharding import PartitionSpec as P

EPS = 1e-06
BF = jnp.bfloat16
F32 = jnp.float32
LOW = -1e30
VL = 56


def device_of(head, part):
    z, pair = divmod(head, 2)
    side, core = divmod(part, 2)
    x = (0, 1, 3, 2)[pair * 2 + side]
    return z * 8 + x * 2 + core


HEAD_GROUPS = [[device_of(g, p) for g in range(16)] for p in range(4)]
CORE_SWAP = [(d, d ^ 1) for d in range(64)]
SIDE_SWAP = [(d, d ^ 2) for d in range(64)]
BOTH_SWAP = [(d, d ^ 3) for d in range(64)]


def to_heads(array):
    return lax.all_to_all(array, "seq", 0, 0, tiled=True, axis_index_groups=HEAD_GROUPS)


def dot_nt(a, b):
    return lax.dot_general(a, b, (((1,), (1,)), ((), ())), preferred_element_type=F32)


def dot_nn(a, b):
    return jnp.dot(a, b, preferred_element_type=F32)


def repeated(x, n):
    return x if n == 1 else jnp.concatenate([x] * n, axis=1)


def pack_kernel(levels, mine, q, k, v, history, out, packed):
    @pl.when(pl.program_id(0) == 0)
    def _():
        level = levels[mine[0]]
        lane_channel = lax.broadcasted_iota(jnp.int32, (16, 128), 1) % 16
        spread = (lane_channel == lax.broadcasted_iota(jnp.int32, (16, 128), 0)).astype(BF)
        tiled = lax.dot_general(
            history[...], spread, (((0,), (0,)), ((), ())), preferred_element_type=F32
        )

        def row_and_piece(pos):
            row = jnp.where(
                level == 2,
                pos % 16 // 2,
                jnp.where(level == 4, pos % 32 // 4, pos % 16 // 8 * 4 + pos // 16),
            )
            piece = jnp.where(
                level == 2,
                pos // 16 * 2 + pos % 2,
                jnp.where(level == 4, pos // 32 * 4 + pos % 4, pos % 8),
            )
            return row, piece

        _, piece = row_and_piece(lax.broadcasted_iota(jnp.int32, (64, 128), 0))
        lane_piece = lax.broadcasted_iota(jnp.int32, (64, 128), 1) // 16
        kept = jnp.where(piece == lane_piece, tiled, 0.0).astype(BF)
        row, _ = row_and_piece(lax.broadcasted_iota(jnp.int32, (8, 64), 1))
        pick = (row == lax.broadcasted_iota(jnp.int32, (8, 64), 0)).astype(BF)
        packed[...] = dot_nn(pick, kept).astype(BF)

    for h in range(8):
        cols = slice(h * 128, (h + 1) * 128)
        out[h, 0:128, :] = q[:, cols]
        out[h, 128:256, :] = k[:, cols]
        out[h, 256:384, :] = v[:, cols]
        out[h, 384:392, :] = packed[...]


def pack(levels, mine, queries, keys, values, history):
    spec = pl.BlockSpec((128, 1024), lambda i, *_: (0, i))
    return pl.pallas_call(
        pack_kernel,
        grid_spec=pltpu.PrefetchScalarGridSpec(
            num_scalar_prefetch=2,
            grid=(2,),
            in_specs=[spec, spec, spec, pl.BlockSpec((16, 64), lambda i, *_: (0, 0))],
            out_specs=pl.BlockSpec((8, 392, 128), lambda i, *_: (i, 0, 0)),
            scratch_shapes=[pltpu.VMEM((8, 128), BF)],
        ),
        out_shape=jax.ShapeDtypeStruct((16, 392, 128), BF),
        compiler_params=pltpu.CompilerParams(dimension_semantics=("arbitrary",)),
    )(levels, mine, queries, keys, values, history)


def history_kernel(heard, rank, patches, scale, shift, weight, out):
    raw = heard[...].reshape(512, 128)
    place = lax.broadcasted_iota(jnp.int32, (512, 512), 0) == rank[...]
    tokens = dot_nn(place.astype(BF), raw).astype(BF)
    gain = 1.0 + scale[...]
    bias = shift[...]
    lane = lax.broadcasted_iota(jnp.int32, (128, 128), 1)

    def finish(total, slot):
        hidden = total.astype(BF).astype(F32)
        width = hidden.shape[1]
        mean = jnp.sum(hidden, axis=1, keepdims=True) * (1.0 / width)
        centered = hidden - mean
        var = jnp.sum(centered * centered, axis=1, keepdims=True) * (1.0 / width)
        normed = (centered * lax.rsqrt(var + EPS) * gain + bias).astype(BF)
        out[:, slot * 128 : (slot + 1) * 128] = lax.dot_general(
            weight[...], normed, (((0,), (1,)), ((), ())), preferred_element_type=F32
        ).astype(BF)

    def part(first, lanes, index):
        block = tokens[first : first + 128, :]
        return jnp.where(lane // lanes == index, block, jnp.zeros_like(block))

    for i in range(4):
        finish(dot_nn(part(0, 32, i), patches[0:128, :]), i)
    for i in range(4):
        finish(dot_nn(part(128 + 128 * (i // 2), 64, i % 2), patches[128:256, :]), 4 + i)
    block = tokens[384:512, :]
    early = dot_nn(block, patches[256:384, :])
    late = dot_nn(block, patches[384:512, :])
    late = jnp.concatenate([late[4:], late[:4]], axis=0)
    finish(early + late, 8)


def history_share(heard, rank, patches, scale, shift, weight):
    full = lambda *shape: pl.BlockSpec(shape, lambda i: (0,) * len(shape))
    return pl.pallas_call(
        history_kernel,
        grid=(1,),
        in_specs=[
            full(4, 16, 8, 128),
            full(1, 512),
            full(512, 3072),
            full(1, 3072),
            full(1, 3072),
            full(3072, 64),
        ],
        out_specs=full(64, 1152),
        out_shape=jax.ShapeDtypeStruct((64, 1152), BF),
        compiler_params=pltpu.CompilerParams(vmem_limit_bytes=40 << 20),
        cost_estimate=pl.CostEstimate(
            flops=8_000_000_000, transcendentals=1152, bytes_accessed=4_000_000
        ),
    )(heard, rank, patches, scale[None], shift[None], weight)


def attend_kernel(cfg, *refs):
    pairs, with_hist, first, last, scale, block = cfg
    refs = list(refs)
    q_ref = refs.pop(0)
    kv = [(refs.pop(0), refs.pop(0)) for _ in range(pairs)]
    if with_hist:
        hist_ref = refs.pop(0)
        gain_ref = refs.pop(0)
    if not first:
        stats_in, acc_in = refs.pop(0), refs.pop(0)
    if last:
        out_ref = refs.pop(0)
    else:
        stats_out, acc_out = refs.pop(0), refs.pop(0)
    if with_hist:
        hist_keys, hist_vals = refs.pop(0), refs.pop(0)

        @pl.when(pl.program_id(0) == 0)
        def _():
            row = lax.broadcasted_iota(jnp.int32, (256, 256), 0)
            col = lax.broadcasted_iota(jnp.int32, (256, 256), 1)
            source = row % 128 // 2 * 4 + row // 128 * 2 + row % 2
            raw = dot_nn((source == col).astype(BF), hist_ref[...])
            keys = raw[0:128, :]
            mean = jnp.sum(keys * keys, axis=0, keepdims=True) * (1.0 / 128)
            gain = jnp.broadcast_to(gain_ref[...], (128, 128)).T[:, 0:1]
            normed = (keys * lax.rsqrt(mean + EPS) * gain).astype(BF)
            hist_keys[0:128, :] = normed
            hist_keys[128:256, :] = normed
            hist_vals[0:128, :] = raw[128:256, :].astype(BF)
            hist_vals[128:256, :] = jnp.ones((128, 1152), BF)

    q = q_ref[...].reshape(-1, 128)
    rows = q.shape[0]
    scaled = q.astype(F32) * scale
    high = scaled.astype(BF)
    low = (scaled - high.astype(F32)).astype(BF)
    q2 = jnp.concatenate([high, low], axis=1)
    if first:
        top = jnp.full((rows, 128), LOW, F32)
        total = jnp.zeros((rows, 128), F32)
        acc = jnp.zeros((rows, 128), F32)
    else:
        stats = stats_in[...]
        top = jnp.broadcast_to(stats[:, 0:1], (rows, 128))
        total = jnp.broadcast_to(stats[:, 127:128], (rows, 128))
        acc = acc_in[...]

    steps = []
    for k_ref, v_ref in kv:
        for i in range(2048 // block):
            steps.append(("section", k_ref, v_ref, i))
    if with_hist:
        steps.append(("history", 0, 1024, 0))
        steps.append(("history", 1024, 1152, 0))

    def scores(step):
        kind, a, b, i = step
        if kind == "section":
            keys = a[i * block // 128 : (i + 1) * block // 128].reshape(block, 128)
            return dot_nt(q2, jnp.concatenate([keys, keys], axis=1))
        s = dot_nn(q2, hist_keys[:, a:b])
        if b == 1152:
            s = jnp.where(lax.broadcasted_iota(jnp.int32, s.shape, 1) % 8 < 4, s, LOW)
        return s

    def mixed(step, probs):
        kind, a, b, i = step
        if kind == "section":
            vals = b[i * block // 128 : (i + 1) * block // 128].reshape(block, 128)
            return dot_nn(probs, jnp.concatenate([vals, jnp.ones_like(vals)], axis=1))
        return dot_nt(probs, hist_vals[:, a:b])

    ahead = scores(steps[0])
    for n, step in enumerate(steps):
        s = ahead
        if n + 1 < len(steps):
            ahead = scores(steps[n + 1])
        newer = jnp.maximum(top, jnp.max(s, axis=1, keepdims=True))
        probs = jnp.exp2(s - repeated(newer, s.shape[1] // 128)).astype(BF)
        fade = jnp.exp2(top - newer)
        part = mixed(step, probs)
        acc = acc * fade + part[:, :128]
        total = total * fade + part[:, 128:]
        top = newer
    if last:
        out_ref[...] = (acc / total).astype(BF).reshape(out_ref.shape)
    else:
        low_lanes = lax.broadcasted_iota(jnp.int32, (rows, 128), 1) < 64
        stats_out[...] = jnp.where(low_lanes, top, total)
        acc_out[...] = acc


def attend(q_array, kvs, state, hist, gain, scale, block=1024):
    first = state is None
    last = hist is not None
    tile = 4
    rows = tile * 128
    q_map = lambda i: (i, 0, 0)
    state_spec = pl.BlockSpec((rows, 128), lambda i: (i, 0))
    args = [q_array]
    in_specs = [pl.BlockSpec((tile, 128, 128), q_map)]
    for array in kvs:
        args += [array, array]
        in_specs += [
            pl.BlockSpec((16, 128, 128), lambda i: (0, 0, 0)),
            pl.BlockSpec((16, 128, 128), lambda i: (0, 1, 0)),
        ]
    scratch = []
    n_keys = 2048 * len(kvs)
    if last:
        args += [hist, gain]
        in_specs += [
            pl.BlockSpec((256, 1152), lambda i: (0, 0)),
            pl.BlockSpec((1, 128), lambda i: (0, 0)),
        ]
        scratch = [pltpu.VMEM((256, 1152), BF), pltpu.VMEM((256, 1152), BF)]
        n_keys += 1152
    if not first:
        args += list(state)
        in_specs += [state_spec] * 2
    if last:
        out_shape = jax.ShapeDtypeStruct((16, 128, 128), BF)
        out_specs = pl.BlockSpec((tile, 128, 128), q_map)
    else:
        out_shape = [jax.ShapeDtypeStruct((2048, 128), F32)] * 2
        out_specs = [state_spec] * 2
    return pl.pallas_call(
        functools.partial(
            attend_kernel, (len(kvs), hist is not None, first, last, scale, block)
        ),
        grid=(16 // tile,),
        in_specs=in_specs,
        out_specs=out_specs,
        out_shape=out_shape,
        scratch_shapes=scratch,
        compiler_params=pltpu.CompilerParams(
            vmem_limit_bytes=VL << 20, dimension_semantics=("arbitrary",)
        ),
        cost_estimate=pl.CostEstimate(
            flops=8 * 2048 * n_keys * 128,
            transcendentals=2048 * n_keys,
            bytes_accessed=n_keys * 512 + 2048 * 2048,
        ),
    )(*args)


def arrival_rank(levels, mine):
    table = levels.reshape(16, 4)
    fours = table == 4
    second = (jnp.cumsum(fours.astype(jnp.int32), axis=1) == 2).astype(jnp.int32)
    kind = jnp.where(table == 2, 0, jnp.where(fours, 1 + second, 3))
    rank = (kind * 16 + jnp.arange(16, dtype=jnp.int32)[:, None]).reshape(64)
    x = mine % 8 // 2
    part = 2 * ((x == 1) | (x == 2)).astype(jnp.int32) + mine % 2
    first = jnp.array(HEAD_GROUPS, jnp.int32)[part]
    ids = (first[None, :] ^ jnp.arange(4, dtype=jnp.int32)[:, None]).reshape(64)
    same = ids[:, None] == jnp.arange(64, dtype=jnp.int32)[None, :]
    arrived = jnp.sum(jnp.where(same, rank[None, :], 0), axis=1)
    return (arrived[:, None] * 8 + jnp.arange(8, dtype=jnp.int32)[None, :]).reshape(1, 512)


def expanded_patches(patch_two, patch_four, patch_sixteen):
    def by_offset(patch, factor):
        return patch.reshape(16, factor, -1).transpose(1, 0, 2).reshape(16 * factor, -1)

    two = by_offset(patch_two, 2)
    four = by_offset(patch_four, 4)
    return jnp.concatenate([two] * 4 + [four] * 2 + [by_offset(patch_sixteen, 16)], axis=0)


def head_columns(weight):
    col = jnp.arange(64, dtype=jnp.int32)
    source = col % 2 * 32 + col // 2 % 2 * 16 + col // 4
    return dot_nn(weight, (col[:, None] == source[None, :]).astype(BF)).astype(BF)


def shards(
    queries,
    keys,
    values,
    history,
    levels,
    patch_two,
    patch_four,
    patch_sixteen,
    mod_scale,
    mod_shift,
    kv_weight,
    key_gain,
):
    scale = 128 ** (-0.5) * math.log2(math.e)
    mine = lax.axis_index("seq")
    send = pack(levels, mine[None].astype(jnp.int32), queries, keys, values, history)
    rank, patches, weight, got = lax.optimization_barrier(
        (
            arrival_rank(levels, mine),
            expanded_patches(patch_two, patch_four, patch_sixteen),
            head_columns(kv_weight),
            to_heads(send),
        )
    )
    heard = got[:, 384:]
    near = lax.ppermute(heard, "seq", CORE_SWAP)
    across = lax.ppermute(heard, "seq", SIDE_SWAP)
    beyond = lax.ppermute(heard, "seq", BOTH_SWAP)
    near, own = lax.optimization_barrier((near, got[:, 128:384]))
    heard = jnp.stack([heard, near, across, beyond])
    core = lax.ppermute(own, "seq", CORE_SWAP)
    side = lax.ppermute(own, "seq", SIDE_SWAP)
    share = history_share(heard, rank, patches, mod_scale, mod_shift, weight)
    share = jnp.broadcast_to(share.reshape(16, 1, 4, 1152), (16, 4, 4, 1152))
    share, got, own, core = lax.optimization_barrier((share.reshape(64, 4, 1152), got, own, core))
    got_hist = lax.all_to_all(share, "seq", 0, 0, tiled=True)
    state = attend(got, [own, core], None, None, None, scale)
    side, state = lax.optimization_barrier((side, state))
    far = lax.ppermute(side, "seq", CORE_SWAP)
    hist = got_hist.reshape(256, 1152)
    mixed = attend(got, [side, far], state, hist, key_gain[None], scale)
    return to_heads(mixed).transpose(1, 0, 2).reshape(128, 2048)


def solution(mesh):
    return jax.shard_map(
        shards,
        mesh=mesh,
        in_specs=(
            P(("video", "seq"), None),
            P(("video", "seq"), None),
            P(("video", "seq"), None),
            P(None, ("video", "seq")),
            P("video"),
            P(),
            P(),
            P(),
            P(),
            P(),
            P(None, "seq"),
            P(),
        ),
        out_specs=P(("video", "seq"), None),
        check_vma=False,
    )
```
